16 devices in a mesh: model: 16 (over z, y, x, core).
Axes of the slice: x: 2, y: 2, z: 2, core: 2. Of those that a mesh axis runs over, the one named last changes fastest.
Arguments:
- act_in: bfloat16 [4096, 18432], P('model')
- ln_gain: float32 [18432], replicated
- w_q: bfloat16 [18432, 12288], P(None, 'model')
- w_kv: bfloat16 [18432, 512], replicated
- w_o: bfloat16 [12288, 18432], P('model')
- positions: int32 [2048], replicated
Outputs:
- output 1: bfloat16 [4096, 18432], P('model')
- output 2: bfloat16 [4096, 256], replicated
- output 3: bfloat16 [4096, 256], replicated
All inputs are finite; a program needn't handle non-finite values.
Results may differ from the reference program's by a relative error of at most 0.013192.
Values are sent between devices in bfloat16 or wider.
A program may use at most 1 GiB of HBM per device.

```python
import jax
import jax.numpy as jnp
from jax import lax

TOKENS = 4096
SEQ = 2048
D = 18432
HEADS = 48
HEAD = 256
NORM_EPS = 1e-6


def setup_inputs(seed: int = 0) -> dict:
    rng_keys = jax.random.split(jax.random.key(seed), 6)
    act_in = jax.random.normal(rng_keys[0], (TOKENS, D), jnp.float32).astype(jnp.bfloat16)
    ln_gain = jax.random.uniform(rng_keys[1], (D,), jnp.float32, 0.6, 1.4)
    w_q = (jax.random.normal(rng_keys[2], (D, HEADS * HEAD), jnp.float32) * D ** -0.5).astype(jnp.bfloat16)
    w_kv = (jax.random.normal(rng_keys[3], (D, 2 * HEAD), jnp.float32) * D ** -0.5).astype(jnp.bfloat16)
    out_scale = (SEQ / (HEADS * HEAD)) ** 0.5 / 8.0
    w_o = (jax.random.normal(rng_keys[4], (HEADS * HEAD, D), jnp.float32) * out_scale).astype(jnp.bfloat16)
    positions = jax.random.permutation(rng_keys[5], SEQ).astype(jnp.int32)
    return dict(act_in=act_in, ln_gain=ln_gain, w_q=w_q, w_kv=w_kv, w_o=w_o, positions=positions)


def layer_norm(act_rows, gain_vec):
    rows_f32 = act_rows.astype(jnp.float32)
    row_mean = jnp.mean(rows_f32, axis=-1, keepdims=True)
    centered = rows_f32 - row_mean
    variance = jnp.mean(centered * centered, axis=-1, keepdims=True)
    return (centered * lax.rsqrt(variance + NORM_EPS) * gain_vec).astype(jnp.bfloat16)


def reference(act_in, ln_gain, w_q, w_kv, w_o, positions):
    normed = layer_norm(act_in, ln_gain)
    queries = jnp.dot(normed, w_q, preferred_element_type=jnp.float32).astype(jnp.bfloat16)
    kv_proj = jnp.dot(normed, w_kv, preferred_element_type=jnp.float32).astype(jnp.bfloat16)
    k_cache = kv_proj[:, :HEAD]
    v_cache = kv_proj[:, HEAD:]
    n_seq = TOKENS // SEQ
    visible = positions[None, :] <= positions[:, None]
    q_seqs = queries.reshape(n_seq, SEQ, HEADS, HEAD).transpose(0, 2, 1, 3)
    k_seqs = k_cache.reshape(n_seq, SEQ, HEAD)
    v_seqs = v_cache.reshape(n_seq, SEQ, HEAD)

    def one_seq(operands):
        q_blk, k_blk, v_blk = operands

        def one_head(q_head):
            scores = jnp.dot(q_head, k_blk.T, preferred_element_type=jnp.float32) * HEAD ** -0.5
            scores = jnp.where(visible, scores, -1e30)
            attn_prob = jax.nn.softmax(scores, axis=-1).astype(jnp.bfloat16)
            return jnp.dot(attn_prob, v_blk, preferred_element_type=jnp.float32).astype(jnp.bfloat16)

        return lax.map(one_head, q_blk)

    attended = lax.map(one_seq, (q_seqs, k_seqs, v_seqs))
    attended = attended.transpose(0, 2, 1, 3).reshape(TOKENS, HEADS * HEAD)
    y_out = jnp.dot(attended, w_o, preferred_element_type=jnp.float32).astype(jnp.bfloat16)
    return y_out, k_cache, v_cache
```

```python
import functools

import jax
import jax.numpy as jnp
from jax import lax
from jax.experimental import pallas as pl
from jax.experimental.pallas import tpu as pltpu
from jax.sharding import Mesh, PartitionSpec as P

NORM_EPS = 1e-6
SWAP = [(0, 1), (1, 0)]
LN_ROWS = 16
ATT_ROWS = 256
CHUNKS = 2


def norm_kernel(x_ref, g_ref, o_ref):
    rows_f32 = x_ref[...].astype(jnp.float32)
    row_mean = jnp.mean(rows_f32, axis=-1, keepdims=True)
    centered = rows_f32 - row_mean
    variance = jnp.mean(centered * centered, axis=-1, keepdims=True)
    o_ref[...] = (centered * lax.rsqrt(variance + NORM_EPS) * g_ref[...]).astype(jnp.bfloat16)


def layer_norm(x_loc, gain_row, start, rows):
    width = x_loc.shape[1]
    first = start // LN_ROWS
    return pl.pallas_call(
        norm_kernel,
        grid=(rows // LN_ROWS,),
        in_specs=[
            pl.BlockSpec((LN_ROWS, width), lambda i: (first + i, 0)),
            pl.BlockSpec((1, width), lambda i: (0, 0)),
        ],
        out_specs=pl.BlockSpec((LN_ROWS, width), lambda i: (i, 0)),
        out_shape=jax.ShapeDtypeStruct((rows, width), jnp.bfloat16),
        name=f"norm_{start}",
        cost_estimate=pl.CostEstimate(flops=rows * width * 8, bytes_accessed=rows * width * 4, transcendentals=0),
    )(x_loc, gain_row)


def attend_kernel(scale, q_ref, k_ref, v_ref, pos_q_ref, pos_k_ref, o_ref):
    scores = lax.dot_general(q_ref[...], k_ref[0], (((1,), (1,)), ((), ())), preferred_element_type=jnp.float32)
    visible = pos_k_ref[...] <= pos_q_ref[...]
    scores = jnp.where(visible, scores * scale, -1e30)
    weights = jnp.exp(scores - jnp.max(scores, axis=-1, keepdims=True))
    inverse = 1.0 / jnp.sum(weights, axis=-1, keepdims=True)
    probs = (weights * inverse).astype(jnp.bfloat16)
    o_ref[...] = jnp.dot(probs, v_ref[0], preferred_element_type=jnp.float32).astype(jnp.bfloat16)


def attend(queries, k_seqs, v_seqs, pos_q, pos_k):
    n_seq, keys, head_dim = k_seqs.shape
    rows = queries.shape[0] // n_seq
    heads = queries.shape[1] // head_dim
    tiles = rows // ATT_ROWS
    flops = 4 * queries.shape[0] * keys * queries.shape[1]
    q_spec = pl.BlockSpec((ATT_ROWS, head_dim), lambda s, n, r: (s * tiles + r, n))
    kv_spec = pl.BlockSpec((1, keys, head_dim), lambda s, n, r: (s, 0, 0))
    return pl.pallas_call(
        functools.partial(attend_kernel, head_dim ** -0.5),
        grid=(n_seq, heads, tiles),
        in_specs=[
            q_spec,
            kv_spec,
            kv_spec,
            pl.BlockSpec((ATT_ROWS, 1), lambda s, n, r: (r, 0)),
            pl.BlockSpec((1, keys), lambda s, n, r: (0, 0)),
        ],
        out_specs=q_spec,
        out_shape=jax.ShapeDtypeStruct(queries.shape, jnp.bfloat16),
        name="attend",
        cost_estimate=pl.CostEstimate(flops=flops, bytes_accessed=4 * queries.size, transcendentals=queries.shape[0] * heads * keys),
    )(queries, k_seqs, v_seqs, pos_q.reshape(rows, 1), pos_k.reshape(1, keys))


def dot32(a, b):
    return jnp.dot(a, b, preferred_element_type=jnp.float32)


def cube_gather(piece, chips, order):
    chip = lax.axis_index("chip")
    bits = chips.bit_length() - 1
    have = piece.reshape((1,) * bits + piece.shape)
    for bit in order:
        other = lax.ppermute(have, "chip", [(i, i ^ (1 << bit)) for i in range(chips)])
        low = (chip // (1 << bit)) % 2 == 0
        axis = bits - 1 - bit
        have = jnp.concatenate([jnp.where(low, have, other), jnp.where(low, other, have)], axis=axis)
    return have.reshape((chips,) + piece.shape)


def solution(mesh):
    chips = mesh.devices.size // 2
    pair_mesh = Mesh(mesh.devices.reshape(chips, 2), ("chip", "core"))

    def local_step(x_loc, ln_gain, wq_loc, w_kv, wo_loc, positions):
        seq_len = positions.shape[0]
        head_dim = w_kv.shape[1] // 2
        rows, width = x_loc.shape
        core = lax.axis_index("core")
        part = rows // CHUNKS
        gain_row = ln_gain.reshape(1, width)

        normed = [layer_norm(x_loc, gain_row, c * part, part) for c in range(CHUNKS)]
        gathered = [lax.all_gather(n, "chip", axis=0, tiled=True) for n in normed]

        wq_all = jnp.concatenate([wq_loc, lax.ppermute(wq_loc, "core", SWAP)], axis=1)
        wo_all = jnp.concatenate([wo_loc, lax.ppermute(wo_loc, "core", SWAP)], axis=0)

        kv_loc = jnp.concatenate([dot32(n, w_kv).astype(jnp.bfloat16) for n in normed], axis=0)
        edges = (0, 96, 176, rows)
        orders = ((0, 1, 2), (1, 2, 0), (2, 0, 1))
        kv_mine = jnp.concatenate(
            [cube_gather(kv_loc[edges[t]:edges[t + 1]], chips, orders[t]) for t in range(3)], axis=1
        )
        kv_oth = lax.ppermute(kv_mine, "core", SWAP)
        first = jnp.where(core == 0, kv_mine, kv_oth)
        second = jnp.where(core == 0, kv_oth, kv_mine)
        kv_all = jnp.stack([first, second], axis=1).reshape(chips * 2 * rows, 2 * head_dim)
        k_cache = kv_all[:, :head_dim]
        v_cache = kv_all[:, head_dim:]
        n_seq = kv_all.shape[0] // seq_len
        per_seq = chips // n_seq
        k_seqs = k_cache.reshape(n_seq, seq_len, head_dim)
        v_seqs = v_cache.reshape(n_seq, seq_len, head_dim)
        pos_mine = lax.dynamic_index_in_dim(positions.reshape(per_seq, 2, rows), core, axis=1, keepdims=False)

        y_out = jnp.zeros((rows, width), jnp.bfloat16)
        for c in range(CHUNKS):
            pos_q = pos_mine[:, c * part:(c + 1) * part].reshape(per_seq * part)
            queries = dot32(gathered[c], wq_all).astype(jnp.bfloat16)
            att = attend(queries, k_seqs, v_seqs, pos_q, positions)
            y_part = dot32(att, wo_all).astype(jnp.bfloat16)
            y_rows = lax.psum_scatter(y_part, "chip", scatter_dimension=0, tiled=True)
            y_out = lax.dynamic_update_slice(y_out, y_rows, (c * part, 0))
            y_out = lax.optimization_barrier(y_out)
        return y_out, k_cache, v_cache

    both = ("chip", "core")
    return jax.shard_map(
        local_step,
        mesh=pair_mesh,
        in_specs=(P(both, None), P(None), P(None, both), P(None, None), P(both, None), P(None)),
        out_specs=(P(both, None), P(None, None), P(None, None)),
        check_vma=False,
    )
```

```python
import functools

import jax
import jax.numpy as jnp
from jax import lax
from jax.experimental import pallas as pl
from jax.experimental.pallas import tpu as pltpu
from jax.sharding import Mesh, PartitionSpec as P

NORM_EPS = 1e-6
SWAP = [(0, 1), (1, 0)]
LN_ROWS = 16
ATT_ROWS = 256
CHUNKS = 2
GROUP_COLS = 512
SETS = 5


def norm_kernel(x_ref, g_ref, o_ref):
    rows_f32 = x_ref[...].astype(jnp.float32)
    row_mean = jnp.mean(rows_f32, axis=-1, keepdims=True)
    centered = rows_f32 - row_mean
    variance = jnp.mean(centered * centered, axis=-1, keepdims=True)
    o_ref[...] = (centered * lax.rsqrt(variance + NORM_EPS) * g_ref[...]).astype(jnp.bfloat16)


def layer_norm(x_loc, gain_row, start, rows):
    width = x_loc.shape[1]
    first = start // LN_ROWS
    return pl.pallas_call(
        norm_kernel,
        grid=(rows // LN_ROWS,),
        in_specs=[
            pl.BlockSpec((LN_ROWS, width), lambda i: (first + i, 0)),
            pl.BlockSpec((1, width), lambda i: (0, 0)),
        ],
        out_specs=pl.BlockSpec((LN_ROWS, width), lambda i: (i, 0)),
        out_shape=jax.ShapeDtypeStruct((rows, width), jnp.bfloat16),
        name=f"norm_{start}",
        cost_estimate=pl.CostEstimate(flops=rows * width * 8, bytes_accessed=rows * width * 4, transcendentals=0),
    )(x_loc, gain_row)


def attend_kernel(scale, q_ref, k_ref, v_ref, pos_q_ref, pos_k_ref, o_ref):
    scores = lax.dot_general(q_ref[...], k_ref[0], (((1,), (1,)), ((), ())), preferred_element_type=jnp.float32)
    visible = pos_k_ref[...] <= pos_q_ref[...]
    scores = jnp.where(visible, scores * scale, -1e30)
    weights = jnp.exp(scores - jnp.max(scores, axis=-1, keepdims=True))
    inverse = 1.0 / jnp.sum(weights, axis=-1, keepdims=True)
    probs = (weights * inverse).astype(jnp.bfloat16)
    o_ref[...] = jnp.dot(probs, v_ref[0], preferred_element_type=jnp.float32).astype(jnp.bfloat16)


def attend(queries, k_seqs, v_seqs, pos_q, pos_k):
    n_seq, keys, head_dim = k_seqs.shape
    rows = queries.shape[0] // n_seq
    heads = queries.shape[1] // head_dim
    tiles = rows // ATT_ROWS
    flops = 4 * queries.shape[0] * keys * queries.shape[1]
    q_spec = pl.BlockSpec((ATT_ROWS, head_dim), lambda s, n, r: (s * tiles + r, n))
    kv_spec = pl.BlockSpec((1, keys, head_dim), lambda s, n, r: (s, 0, 0))
    return pl.pallas_call(
        functools.partial(attend_kernel, head_dim ** -0.5),
        grid=(n_seq, heads, tiles),
        in_specs=[
            q_spec,
            kv_spec,
            kv_spec,
            pl.BlockSpec((ATT_ROWS, 1), lambda s, n, r: (r, 0)),
            pl.BlockSpec((1, keys), lambda s, n, r: (0, 0)),
        ],
        out_specs=q_spec,
        out_shape=jax.ShapeDtypeStruct(queries.shape, jnp.bfloat16),
        name="attend",
        cost_estimate=pl.CostEstimate(flops=flops, bytes_accessed=4 * queries.size, transcendentals=queries.shape[0] * heads * keys),
    )(queries, k_seqs, v_seqs, pos_q.reshape(rows, 1), pos_k.reshape(1, keys))


def dot32(a, b):
    return jnp.dot(a, b, preferred_element_type=jnp.float32)


def scatter_kernel(iters, att_ref, w_ref, o_ref, y, got1, got2, got3, w_buf, w_sem, send1, send2, send3, recv1, recv2, recv3):
    chip = lax.axis_index("chip")
    mine = [(chip // p) % 2 for p in (1, 2, 4)]
    peer = [chip + p - 2 * p * mine[b] for b, p in enumerate((1, 2, 4))]
    gots, sends, recvs = (got1, got2, got3), (send1, send2, send3), (recv1, recv2, recv3)

    barrier = pltpu.get_barrier_semaphore()
    for b in range(3):
        pl.semaphore_signal(barrier, inc=1, device_id={"chip": peer[b]}, device_id_type=pl.DeviceIdType.MESH)
    pl.semaphore_wait(barrier, 3)

    def slot_of(i, j):
        return lax.rem(i, SETS) * 3 + j

    def region(i, j, step, keep):
        index = [slice(None)] * 3
        for s in range(step + 1):
            b = (j + s) % 3
            index[2 - b] = mine[b] if (s < step or keep) else 1 - mine[b]
        return (slot_of(i, j),) + tuple(index)

    def remote(i, j, step):
        slot = slot_of(i, j)
        return pltpu.make_async_remote_copy(
            src_ref=y.at[region(i, j, step, False)],
            dst_ref=gots[step].at[slot],
            send_sem=sends[step].at[slot],
            recv_sem=recvs[step].at[slot],
            device_id={"chip": peer[(j + step) % 3]},
            device_id_type=pl.DeviceIdType.MESH,
        )

    def w_copy(i, j):
        col = pl.multiple_of((i * 3 + j) * GROUP_COLS, GROUP_COLS)
        return pltpu.make_async_copy(w_ref.at[:, pl.ds(col, GROUP_COLS)], w_buf.at[j], w_sem.at[j])

    def add(i, j, step):
        slot = slot_of(i, j)
        free = 2 - step
        for n in range(2 ** free):
            local = [(n >> (free - 1 - d)) % 2 for d in range(free)]
            index, left = [None] * 3, list(local)
            for s in range(step + 1):
                b = (j + s) % 3
                index[2 - b] = mine[b]
            for axis in range(3):
                if index[axis] is None:
                    index[axis] = left.pop(0)
            kept = y[(slot,) + tuple(index)].astype(jnp.float32)
            total = (kept + gots[step][(slot,) + tuple(local)].astype(jnp.float32)).astype(jnp.bfloat16)
            if step < 2:
                y[(slot,) + tuple(index)] = total
            else:
                col = pl.multiple_of((i * 3 + j) * GROUP_COLS, GROUP_COLS)
                o_ref[:, pl.ds(col, GROUP_COLS)] = total

    for j in range(3):
        w_copy(0, j).start()

    def body(i, carry):
        @pl.when(i < iters)
        def _():
            for j in range(3):
                w_copy(i, j).wait()
                for r in range(4):
                    rows = 2 * y.shape[4]
                    out = jnp.dot(att_ref[r * rows:(r + 1) * rows, :], w_buf[j], preferred_element_type=jnp.float32)
                    out = out.astype(jnp.bfloat16)
                    y[slot_of(i, j), r // 2, r % 2, 0] = out[:rows // 2]
                    y[slot_of(i, j), r // 2, r % 2, 1] = out[rows // 2:]

                @pl.when(i + 1 < iters)
                def _():
                    w_copy(i + 1, j).start()

                if j > 0:
                    remote(i, j - 1, 0).start()

        for step in range(3):
            at = i - 2 - step

            @pl.when((at >= 0) & (at < iters))
            def _():
                for j in range(3):
                    remote(at, j, step).wait_recv()
                    add(at, j, step)
                    if j > 0 and step < 2:
                        remote(at, j - 1, step + 1).start()
                    if step == 2:
                        for s in range(3):
                            remote(at, j, s).wait_send()

            if step == 0:
                @pl.when(i < iters)
                def _():
                    remote(i, 2, 0).start()

            if step > 0:
                @pl.when((i - 1 - step >= 0) & (i - 1 - step < iters))
                def _():
                    remote(i - 1 - step, 2, step).start()

        return carry

    lax.fori_loop(0, iters + 4, body, 0)


def project_scatter(att, wo_all, chips):
    rows, width = att.shape[0] // chips, wo_all.shape[1]
    iters = width // (3 * GROUP_COLS)
    block = (rows, GROUP_COLS)
    slots = 3 * SETS
    return pl.pallas_call(
        functools.partial(scatter_kernel, iters),
        out_shape=jax.ShapeDtypeStruct((rows, width), jnp.bfloat16),
        in_specs=[pl.BlockSpec(memory_space=pltpu.VMEM), pl.BlockSpec(memory_space=pl.ANY)],
        out_specs=pl.BlockSpec(memory_space=pltpu.VMEM),
        scratch_shapes=[
            pltpu.VMEM((slots, 2, 2, 2) + block, jnp.bfloat16),
            pltpu.VMEM((slots, 2, 2) + block, jnp.bfloat16),
            pltpu.VMEM((slots, 2) + block, jnp.bfloat16),
            pltpu.VMEM((slots,) + block, jnp.bfloat16),
            pltpu.VMEM((3, wo_all.shape[0], GROUP_COLS), jnp.bfloat16),
            pltpu.SemaphoreType.DMA((3,)),
        ] + [pltpu.SemaphoreType.DMA((slots,)) for _ in range(6)],
        compiler_params=pltpu.CompilerParams(collective_id=0, has_side_effects=True, vmem_limit_bytes=60 * 2 ** 20),
        name="project_scatter",
        cost_estimate=pl.CostEstimate(flops=2 * att.size * width, bytes_accessed=2 * wo_all.size, transcendentals=0),
    )(att, wo_all)


def cube_gather(piece, chips, order):
    chip = lax.axis_index("chip")
    bits = chips.bit_length() - 1
    have = piece.reshape((1,) * bits + piece.shape)
    for bit in order:
        other = lax.ppermute(have, "chip", [(i, i ^ (1 << bit)) for i in range(chips)])
        low = (chip // (1 << bit)) % 2 == 0
        axis = bits - 1 - bit
        have = jnp.concatenate([jnp.where(low, have, other), jnp.where(low, other, have)], axis=axis)
    return have.reshape((chips,) + piece.shape)


def solution(mesh):
    chips = mesh.devices.size // 2
    pair_mesh = Mesh(mesh.devices.reshape(chips, 2), ("chip", "core"))

    def local_step(x_loc, ln_gain, wq_loc, w_kv, wo_loc, positions):
        seq_len = positions.shape[0]
        head_dim = w_kv.shape[1] // 2
        rows, width = x_loc.shape
        core = lax.axis_index("core")
        part = rows // CHUNKS
        gain_row = ln_gain.reshape(1, width)

        normed = [layer_norm(x_loc, gain_row, c * part, part) for c in range(CHUNKS)]
        gathered = [lax.all_gather(n, "chip", axis=0, tiled=True) for n in normed]

        wq_all = jnp.concatenate([wq_loc, lax.ppermute(wq_loc, "core", SWAP)], axis=1)
        wo_all = jnp.concatenate([wo_loc, lax.ppermute(wo_loc, "core", SWAP)], axis=0)

        kv_loc = jnp.concatenate([dot32(n, w_kv).astype(jnp.bfloat16) for n in normed], axis=0)
        edges = (0, 96, 176, rows)
        orders = ((0, 1, 2), (1, 2, 0), (2, 0, 1))
        kv_mine = jnp.concatenate(
            [cube_gather(kv_loc[edges[t]:edges[t + 1]], chips, orders[t]) for t in range(3)], axis=1
        )
        kv_oth = lax.ppermute(kv_mine, "core", SWAP)
        first = jnp.where(core == 0, kv_mine, kv_oth)
        second = jnp.where(core == 0, kv_oth, kv_mine)
        kv_all = jnp.stack([first, second], axis=1).reshape(chips * 2 * rows, 2 * head_dim)
        k_cache = kv_all[:, :head_dim]
        v_cache = kv_all[:, head_dim:]
        n_seq = kv_all.shape[0] // seq_len
        per_seq = chips // n_seq
        k_seqs = k_cache.reshape(n_seq, seq_len, head_dim)
        v_seqs = v_cache.reshape(n_seq, seq_len, head_dim)
        pos_mine = lax.dynamic_index_in_dim(positions.reshape(per_seq, 2, rows), core, axis=1, keepdims=False)

        y_out = jnp.zeros((rows, width), jnp.bfloat16)
        for c in range(CHUNKS):
            pos_q = pos_mine[:, c * part:(c + 1) * part].reshape(per_seq * part)
            queries = dot32(gathered[c], wq_all).astype(jnp.bfloat16)
            att = attend(queries, k_seqs, v_seqs, pos_q, positions)
            if c + 1 < CHUNKS:
                y_part = dot32(att, wo_all).astype(jnp.bfloat16)
                y_rows = lax.psum_scatter(y_part, "chip", scatter_dimension=0, tiled=True)
            else:
                y_rows = project_scatter(att, wo_all, chips)
            y_out = lax.dynamic_update_slice(y_out, y_rows, (c * part, 0))
            y_out = lax.optimization_barrier(y_out)
        return y_out, k_cache, v_cache

    both = ("chip", "core")
    return jax.shard_map(
        local_step,
        mesh=pair_mesh,
        in_specs=(P(both, None), P(None), P(None, both), P(None, None), P(both, None), P(None)),
        out_specs=(P(both, None), P(None, None), P(None, None)),
        check_vma=False,
    )
```

```python
import functools

import jax
import jax.numpy as jnp
from jax import lax
from jax.experimental import pallas as pl
from jax.experimental.pallas import tpu as pltpu
from jax.sharding import Mesh, PartitionSpec as P


NORM_EPS = 1e-6
SWAP = [(0, 1), (1, 0)]
LN_ROWS = 16
GATHER_GROUPS = 6
GROUP_COLS = 512
SETS = 5


def normalized(rows_bf16, gain_row):
    rows_f32 = rows_bf16.astype(jnp.float32)
    row_mean = jnp.mean(rows_f32, axis=-1, keepdims=True)
    centered = rows_f32 - row_mean
    variance = jnp.mean(centered * centered, axis=-1, keepdims=True)
    return (centered * lax.rsqrt(variance + NORM_EPS) * gain_row).astype(jnp.bfloat16)


def norm_kernel(x_ref, g_ref, o_ref):
    o_ref[...] = normalized(x_ref[...], g_ref[...])


def layer_norm(x_loc, gain_row, start, rows):
    width = x_loc.shape[1]
    first = start // LN_ROWS
    return pl.pallas_call(
        norm_kernel,
        grid=(rows // LN_ROWS,),
        in_specs=[
            pl.BlockSpec((LN_ROWS, width), lambda i: (first + i, 0)),
            pl.BlockSpec((1, width), lambda i: (0, 0)),
        ],
        out_specs=pl.BlockSpec((LN_ROWS, width), lambda i: (i, 0)),
        out_shape=jax.ShapeDtypeStruct((rows, width), jnp.bfloat16),
        cost_estimate=pl.CostEstimate(flops=rows * width * 8, bytes_accessed=rows * width * 4, transcendentals=0),
    )(x_loc, gain_row)


def attend_kernel(scale, q_ref, k_ref, v_ref, pos_q_ref, pos_k_ref, o_ref):
    scores = lax.dot_general(q_ref[...], k_ref[0], (((1,), (1,)), ((), ())), preferred_element_type=jnp.float32)
    visible = pos_k_ref[...] <= pos_q_ref[...]
    scores = jnp.where(visible, scores * scale, -1e30)
    weights = jnp.exp(scores - jnp.max(scores, axis=-1, keepdims=True))
    inverse = 1.0 / jnp.sum(weights, axis=-1, keepdims=True)
    probs = (weights * inverse).astype(jnp.bfloat16)
    o_ref[...] = jnp.dot(probs, v_ref[0], preferred_element_type=jnp.float32).astype(jnp.bfloat16)


def attend(queries, k_seqs, v_seqs, pos_q, pos_k, tiles):
    n_seq, keys, head_dim = k_seqs.shape
    rows = queries.shape[0] // n_seq
    heads = queries.shape[1] // head_dim
    tile = rows // tiles
    flops = 4 * queries.shape[0] * keys * queries.shape[1]
    q_spec = pl.BlockSpec((tile, head_dim), lambda s, n, r: (s * tiles + r, n))
    kv_spec = pl.BlockSpec((1, keys, head_dim), lambda s, n, r: (s, 0, 0))
    return pl.pallas_call(
        functools.partial(attend_kernel, head_dim ** -0.5),
        grid=(n_seq, heads, tiles),
        in_specs=[
            q_spec,
            kv_spec,
            kv_spec,
            pl.BlockSpec((tile, 1), lambda s, n, r: (r, 0)),
            pl.BlockSpec((1, keys), lambda s, n, r: (0, 0)),
        ],
        out_specs=q_spec,
        out_shape=jax.ShapeDtypeStruct(queries.shape, jnp.bfloat16),
        name="attend",
        cost_estimate=pl.CostEstimate(flops=flops, bytes_accessed=4 * queries.size, transcendentals=queries.shape[0] * heads * keys),
    )(queries, k_seqs, v_seqs, pos_q.reshape(rows, 1), pos_k.reshape(1, keys))


def dot32(a, b):
    return jnp.dot(a, b, preferred_element_type=jnp.float32)


def scatter_kernel(iters, att_ref, w_ref, o_ref, y, got1, got2, got3, w_buf, w_sem, send1, send2, send3, recv1, recv2, recv3):
    chip = lax.axis_index("chip")
    mine = [(chip // p) % 2 for p in (1, 2, 4)]
    peer = [chip + p - 2 * p * mine[b] for b, p in enumerate((1, 2, 4))]
    gots, sends, recvs = (got1, got2, got3), (send1, send2, send3), (recv1, recv2, recv3)

    barrier = pltpu.get_barrier_semaphore()
    for b in range(3):
        pl.semaphore_signal(barrier, inc=1, device_id={"chip": peer[b]}, device_id_type=pl.DeviceIdType.MESH)
    pl.semaphore_wait(barrier, 3)

    def slot_of(i, j):
        return lax.rem(i, SETS) * 3 + j

    def region(i, j, step, keep):
        index = [slice(None)] * 3
        for s in range(step + 1):
            b = (j + s) % 3
            index[2 - b] = mine[b] if (s < step or keep) else 1 - mine[b]
        return (slot_of(i, j),) + tuple(index)

    def remote(i, j, step):
        slot = slot_of(i, j)
        return pltpu.make_async_remote_copy(
            src_ref=y.at[region(i, j, step, False)],
            dst_ref=gots[step].at[slot],
            send_sem=sends[step].at[slot],
            recv_sem=recvs[step].at[slot],
            device_id={"chip": peer[(j + step) % 3]},
            device_id_type=pl.DeviceIdType.MESH,
        )

    def w_copy(i, j):
        col = pl.multiple_of((i * 3 + j) * GROUP_COLS, GROUP_COLS)
        return pltpu.make_async_copy(w_ref.at[:, pl.ds(col, GROUP_COLS)], w_buf.at[j], w_sem.at[j])

    def add(i, j, step):
        slot = slot_of(i, j)
        free = 2 - step
        for n in range(2 ** free):
            local = [(n >> (free - 1 - d)) % 2 for d in range(free)]
            index, left = [None] * 3, list(local)
            for s in range(step + 1):
                b = (j + s) % 3
                index[2 - b] = mine[b]
            for axis in range(3):
                if index[axis] is None:
                    index[axis] = left.pop(0)
            kept = y[(slot,) + tuple(index)].astype(jnp.float32)
            total = (kept + gots[step][(slot,) + tuple(local)].astype(jnp.float32)).astype(jnp.bfloat16)
            if step < 2:
                y[(slot,) + tuple(index)] = total
            else:
                col = pl.multiple_of((i * 3 + j) * GROUP_COLS, GROUP_COLS)
                o_ref[:, pl.ds(col, GROUP_COLS)] = total

    for j in range(3):
        w_copy(0, j).start()

    def body(i, carry):
        @pl.when(i < iters)
        def _():
            for j in range(3):
                w_copy(i, j).wait()
                for r in range(4):
                    rows = 2 * y.shape[4]
                    out = jnp.dot(att_ref[r * rows:(r + 1) * rows, :], w_buf[j], preferred_element_type=jnp.float32)
                    out = out.astype(jnp.bfloat16)
                    y[slot_of(i, j), r // 2, r % 2, 0] = out[:rows // 2]
                    y[slot_of(i, j), r // 2, r % 2, 1] = out[rows // 2:]

                @pl.when(i + 1 < iters)
                def _():
                    w_copy(i + 1, j).start()

                if j > 0:
                    remote(i, j - 1, 0).start()

        for step in range(3):
            at = i - 2 - step

            @pl.when((at >= 0) & (at < iters))
            def _():
                for j in range(3):
                    remote(at, j, step).wait_recv()
                    add(at, j, step)
                    if j > 0 and step < 2:
                        remote(at, j - 1, step + 1).start()
                    if step == 2:
                        for s in range(3):
                            remote(at, j, s).wait_send()

            if step == 0:
                @pl.when(i < iters)
                def _():
                    remote(i, 2, 0).start()

            if step > 0:
                @pl.when((i - 1 - step >= 0) & (i - 1 - step < iters))
                def _():
                    remote(i - 1 - step, 2, step).start()

        return carry

    lax.fori_loop(0, iters + 4, body, 0)


def gather_kernel(piece_ref, x_ref, g_ref, o_ref, next_ref, own_sem, send_sems, recv_sems):
    chip = lax.axis_index("chip")
    mine = [(chip // p) % 2 for p in (1, 2, 4)]
    peer = [chip + p - 2 * p * mine[b] for b, p in enumerate((1, 2, 4))]
    cols = piece_ref.shape[1] // GATHER_GROUPS
    own = pltpu.make_async_copy(piece_ref, o_ref.at[mine[2], mine[1], mine[0]], own_sem)
    own.start()

    barrier = pltpu.get_barrier_semaphore()
    for b in range(3):
        pl.semaphore_signal(barrier, inc=1, device_id={"chip": peer[b]}, device_id_type=pl.DeviceIdType.MESH)
    pl.semaphore_wait(barrier, 3)

    def remote(g, step):
        index = [None] * 3
        for s in range(3):
            b = (g + s) % 3
            index[2 - b] = slice(None) if s < step else mine[b]
        where = tuple(index) + (slice(None), slice(g * cols, (g + 1) * cols))
        source = piece_ref.at[:, g * cols:(g + 1) * cols] if step == 0 else o_ref.at[where]
        return pltpu.make_async_remote_copy(
            src_ref=source,
            dst_ref=o_ref.at[where],
            send_sem=send_sems.at[step, g],
            recv_sem=recv_sems.at[step, g],
            device_id={"chip": peer[(g + step) % 3]},
            device_id_type=pl.DeviceIdType.MESH,
        )

    for step in range(3):
        for g in range(GATHER_GROUPS):
            if step > 0:
                remote(g, step - 1).wait_recv()
            remote(g, step).start()
        if step == 0:
            def norm_rows(r, carry):
                at = pl.ds(pl.multiple_of(r * LN_ROWS, LN_ROWS), LN_ROWS)
                next_ref[at, :] = normalized(x_ref[at, :], g_ref[...])
                return carry

            lax.fori_loop(0, x_ref.shape[0] // LN_ROWS, norm_rows, 0)
            own.wait()
    for g in range(GATHER_GROUPS):
        remote(g, 2).wait_recv()
        for step in range(3):
            remote(g, step).wait_send()


def kernel_gather(piece, x_loc, gain_row, chips):
    rows, width = piece.shape
    out, following = pl.pallas_call(
        gather_kernel,
        grid=(1,),
        out_shape=(
            jax.ShapeDtypeStruct((2, 2, 2, rows, width), piece.dtype),
            jax.ShapeDtypeStruct((rows, width), piece.dtype),
        ),
        in_specs=[
            pl.BlockSpec((rows, width), lambda i: (0, 0), pipeline_mode=pl.Buffered(1)),
            pl.BlockSpec((rows, width), lambda i: (1, 0), pipeline_mode=pl.Buffered(1)),
            pl.BlockSpec((1, width), lambda i: (0, 0), pipeline_mode=pl.Buffered(1)),
        ],
        out_specs=(
            pl.BlockSpec(memory_space=pl.ANY),
            pl.BlockSpec((rows, width), lambda i: (0, 0), pipeline_mode=pl.Buffered(1)),
        ),
        scratch_shapes=[
            pltpu.SemaphoreType.DMA,
            pltpu.SemaphoreType.DMA((3, GATHER_GROUPS)),
            pltpu.SemaphoreType.DMA((3, GATHER_GROUPS)),
        ],
        compiler_params=pltpu.CompilerParams(collective_id=1, has_side_effects=True, vmem_limit_bytes=48 * 2 ** 20),
        name="kernel_gather",
        cost_estimate=pl.CostEstimate(flops=10 ** 10, bytes_accessed=8 * piece.size, transcendentals=0),
    )(piece, x_loc, gain_row)
    return out.reshape(chips * rows, width), following


def project_scatter(att, wo_all, chips):
    rows, width = att.shape[0] // chips, wo_all.shape[1]
    iters = width // (3 * GROUP_COLS)
    block = (rows, GROUP_COLS)
    slots = 3 * SETS
    return pl.pallas_call(
        functools.partial(scatter_kernel, iters),
        out_shape=jax.ShapeDtypeStruct((rows, width), jnp.bfloat16),
        in_specs=[pl.BlockSpec(memory_space=pltpu.VMEM), pl.BlockSpec(memory_space=pl.ANY)],
        out_specs=pl.BlockSpec(memory_space=pltpu.VMEM),
        scratch_shapes=[
            pltpu.VMEM((slots, 2, 2, 2) + block, jnp.bfloat16),
            pltpu.VMEM((slots, 2, 2) + block, jnp.bfloat16),
            pltpu.VMEM((slots, 2) + block, jnp.bfloat16),
            pltpu.VMEM((slots,) + block, jnp.bfloat16),
            pltpu.VMEM((3, wo_all.shape[0], GROUP_COLS), jnp.bfloat16),
            pltpu.SemaphoreType.DMA((3,)),
        ] + [pltpu.SemaphoreType.DMA((slots,)) for _ in range(6)],
        compiler_params=pltpu.CompilerParams(collective_id=0, has_side_effects=True, vmem_limit_bytes=60 * 2 ** 20),
        name="project_scatter",
        cost_estimate=pl.CostEstimate(flops=2 * att.size * width, bytes_accessed=2 * wo_all.size, transcendentals=0),
    )(att, wo_all)


def cube_gather(piece, chips, order):
    chip = lax.axis_index("chip")
    bits = chips.bit_length() - 1
    have = piece.reshape((1,) * bits + piece.shape)
    for bit in order:
        other = lax.ppermute(have, "chip", [(i, i ^ (1 << bit)) for i in range(chips)])
        low = (chip // (1 << bit)) % 2 == 0
        axis = bits - 1 - bit
        have = jnp.concatenate([jnp.where(low, have, other), jnp.where(low, other, have)], axis=axis)
    return have.reshape((chips,) + piece.shape)


def solution(mesh):
    chips = mesh.devices.size // 2
    pair_mesh = Mesh(mesh.devices.reshape(chips, 2), ("chip", "core"))

    def layer(x_loc, ln_gain, wq_loc, w_kv, wo_loc, positions):
        seq_len = positions.shape[0]
        head_dim = w_kv.shape[1] // 2
        rows, width = x_loc.shape
        core = lax.axis_index("core")
        part = rows // 2
        gain_row = ln_gain.reshape(1, width)

        n_a = layer_norm(x_loc, gain_row, 0, part)
        h_a, n_b = kernel_gather(n_a, x_loc, gain_row, chips)
        h_b = lax.all_gather(n_b, "chip", axis=0, tiled=True)
        n_a, h_a = lax.optimization_barrier((n_a, h_a))

        wq_both = (wq_loc, lax.ppermute(wq_loc, "core", SWAP))
        wo_oth = lax.ppermute(wo_loc, "core", SWAP)
        wo_all = jnp.concatenate([wo_loc, wo_oth], axis=0)

        kv_loc = jnp.concatenate([dot32(n, w_kv).astype(jnp.bfloat16) for n in (n_a, n_b)], axis=0)
        edges = (0, 96, 176, rows)
        orders = ((0, 1, 2), (1, 2, 0), (2, 0, 1))
        kv_mine = jnp.concatenate(
            [cube_gather(kv_loc[edges[t]:edges[t + 1]], chips, orders[t]) for t in range(3)], axis=1
        )
        kv_oth = lax.ppermute(kv_mine, "core", SWAP)
        first = jnp.where(core == 0, kv_mine, kv_oth)
        second = jnp.where(core == 0, kv_oth, kv_mine)
        kv_all = jnp.stack([first, second], axis=1).reshape(chips * 2 * rows, 2 * head_dim)
        k_cache = kv_all[:, :head_dim]
        v_cache = kv_all[:, head_dim:]
        n_seq = kv_all.shape[0] // seq_len
        per_seq = chips // n_seq
        k_seqs = k_cache.reshape(n_seq, seq_len, head_dim)
        v_seqs = v_cache.reshape(n_seq, seq_len, head_dim)
        pos_mine = lax.dynamic_index_in_dim(positions.reshape(per_seq, 2, rows), core, axis=1, keepdims=False)

        def attended(h, start):
            queries = []
            for w in wq_both:
                queries.append(dot32(h, w).astype(jnp.bfloat16))
            queries = jnp.concatenate(queries, axis=1)
            pos_q = pos_mine[:, start:start + part].reshape(per_seq * part)
            return attend(queries, k_seqs, v_seqs, pos_q, positions, 2)

        y_a = dot32(attended(h_a, 0), wo_all).astype(jnp.bfloat16)
        r_a = lax.psum_scatter(y_a, "chip", scatter_dimension=0, tiled=True)
        r_b = project_scatter(attended(h_b, part), wo_all, chips)
        y_out = jnp.zeros((rows, width), jnp.bfloat16)
        y_out = lax.optimization_barrier(lax.dynamic_update_slice(y_out, r_a, (0, 0)))
        y_out = lax.dynamic_update_slice(y_out, r_b, (part, 0))
        return y_out, k_cache, v_cache

    both = ("chip", "core")
    return jax.shard_map(
        layer,
        mesh=pair_mesh,
        in_specs=(P(both, None), P(None), P(None, both), P(None, None), P(both, None), P(None)),
        out_specs=(P(both, None), P(None, None), P(None, None)),
        check_vma=False,
    )
```
